32 devices in a mesh: pop: 2 (over x), snp: 16 (over z, y, core).
Axes of the slice: x: 2, y: 2, z: 4, core: 2. Of those that a mesh axis runs over, the one named last changes fastest.
Arguments:
- genotypes: float32 [4, 1024, 16384], P('pop', None, 'snp'), may hold values from -6 to 6
- pop_id: int32 [4], replicated, may hold values from 0 to 4
- window: int32 [1], replicated, may hold values from 512 to 1024
- tile_counts: int32 [128], P('snp'), may hold values from 64 to 128
- weights: float32 [5, 128], replicated, may hold values from 0.1 to 1
Outputs:
- combined: float32 [16384, 1024], P(('snp', 'pop'))
The draws below stay inside these ranges and needn't reach their ends.
All inputs are finite; a program needn't handle non-finite values.
Results may differ from the reference program's by a relative error of at most 0.000067.
Values sent between devices are 32-bit elements; how exact they have to be, the bound alone decides.
No kernel may reach another device: no remote copies, remote signals or barrier semaphores. Data moves between devices by JAX's collectives and lax.ppermute only.
A program may use at most 128 MiB of HBM per device.

```python
import math
import jax
import jax.numpy as jnp
from jax import lax

IND = 1024
WIN = 1024
NPOPS = 5
COHORTS = 4
SNPS = 16384
TILES = 128


def with_ends(result, key, smallest, largest):
    longest = result.shape.index(max(result.shape))
    spots = []
    for shift in (0, 1):
        where = [jax.random.randint(jax.random.fold_in(key, axis), (), 0, length) for axis, length in enumerate(result.shape)]
        where[longest] = (where[longest] + shift) % result.shape[longest]
        spots.append(tuple(where))
    return result.at[spots[0]].set(smallest).at[spots[1]].set(largest)


def levels(rng, extent, pieces, smallest, largest):
    level = 1.0
    for position, blocks in pieces:
        heights = jax.random.uniform(jax.random.fold_in(jax.random.fold_in(rng, 6), position), (blocks,), jnp.float32, smallest / len(pieces), largest / len(pieces))
        level = level * jnp.repeat(jnp.exp(heights), extent[position] // blocks).reshape((-1,) + (1,) * (len(extent) - 1 - position))
    return level


def bell_draw(own_key, dims, scale, most, cuts=(), kind=jnp.bfloat16):
    values = jax.random.normal(own_key, dims, jnp.float32) * scale
    if len(cuts) > 0:
        values = levels(own_key, dims, cuts, -0.22, 0.18) * values
    return jnp.clip(values, min=-most, max=most).astype(kind)


def setup_inputs(seed: int = 0) -> dict:
    arg_keys = jax.random.split(jax.random.key(seed), 6)
    genotypes = bell_draw(arg_keys[0], (COHORTS, IND, SNPS), 1.0, 6.0, ((0, 2), (2, 16)), jnp.float32)
    pop_id = with_ends(jax.random.randint(arg_keys[1], (COHORTS,), 0, NPOPS), jax.random.fold_in(arg_keys[1], 1), 0, NPOPS - 1).astype(jnp.int32)
    window = jax.random.randint(arg_keys[2], (1,), WIN // 2, WIN + 1).astype(jnp.int32)
    tile_counts = with_ends(jax.random.randint(arg_keys[3], (TILES,), 64, 129), jax.random.fold_in(arg_keys[3], 1), 64, 128).astype(jnp.int32)
    weights = jnp.clip(jnp.exp(jax.random.uniform(arg_keys[4], (NPOPS, TILES), jnp.float32, math.log(0.1), math.log(1.0))), 0.1, 1.0)
    return {"genotypes": genotypes, "pop_id": pop_id, "window": window, "tile_counts": tile_counts, "weights": weights}


def skewed(panel):
    lead = panel.shape[:-2]
    height = panel.shape[-2]
    span = panel.shape[-1] - height
    flat = panel.reshape(lead + (height * (height + span),))
    flat = jnp.concatenate([flat, jnp.zeros(lead + (height,), panel.dtype)], axis=-1)
    return flat.reshape(lead + (height, height + span + 1))[..., :span]


def reference(genotypes, pop_id, window, tile_counts, weights):
    within = jnp.arange(SNPS, dtype=jnp.int32) % 128
    valid = (jnp.repeat(tile_counts, 128) > within).astype(jnp.float32)
    masked = genotypes * valid
    padded = jnp.concatenate([masked, jnp.zeros((COHORTS, IND, WIN), jnp.float32)], axis=2)
    onehot = (pop_id[:, None] == jnp.arange(NPOPS, dtype=jnp.int32)[None, :]).astype(jnp.float32)
    per_cohort = jnp.dot(onehot, weights, precision=lax.Precision.HIGHEST, preferred_element_type=jnp.float32)
    coef = per_cohort / jnp.sum(per_cohort, axis=0, keepdims=True)
    keep = (jnp.arange(WIN, dtype=jnp.int32) < window[0]).astype(jnp.float32)

    def one_tile(tile_index):
        panel = lax.dynamic_slice_in_dim(padded, tile_index * 128, 128 + WIN, 2)
        products = jnp.einsum("cki,ckj->cij", panel[:, :, :128], panel, precision=lax.Precision.HIGHEST) / IND
        band = skewed(products) * keep
        factor = lax.dynamic_slice_in_dim(coef, tile_index, 1, 1)
        return jnp.sum(factor[:, :, None] * band, axis=0)

    tiles_out = lax.map(one_tile, jnp.arange(TILES, dtype=jnp.int32))
    return tiles_out.reshape(SNPS, WIN)
```

```python
import functools

import jax
import jax.numpy as jnp
from jax import lax
from jax.experimental import pallas as pl
from jax.experimental.pallas import tpu as pltpu
from jax.sharding import PartitionSpec as P


WIN = 1024
TILE = 128
STRIP = 256
F32 = jnp.float32
BF16 = jnp.bfloat16
SMEM = pl.BlockSpec(memory_space=pltpu.SMEM)
VMEM = pl.BlockSpec(memory_space=pltpu.VMEM)
PARAMS = pltpu.CompilerParams(vmem_limit_bytes=20 * 2**20)
HOPS = {8: (2, 2, 2, 1, 1), 7: (2, 2, 2, 1), 6: (2, 2, 1, 1), 5: (2, 2, 1)}


class Hop:
    def __init__(self, tile, wide, steps, tiles):
        self.tile, self.wide = tile, wide
        self.first = tile + tiles - steps
        self.base = max(self.first, tiles // 2)
        self.top = max(0, tiles // 2 - self.first) * wide
        self.bottom = (tiles - self.base) * wide
        self.rest = (0, 0)


class Plan:
    def __init__(self, steps, tiles):
        self.steps, self.tiles, self.half = steps, tiles, tiles // 2
        self.counts = [min(steps + 1, tiles - r) for r in range(tiles)]
        starts = [sum(self.counts[:r]) for r in range(tiles + 1)]
        self.n0 = starts[self.half]
        self.n1 = starts[tiles] - self.n0
        self.starts = [s if r < self.half else s - self.n0 for r, s in enumerate(starts[:tiles])]
        self.hops, tile = [], 0
        for wide in HOPS[steps]:
            self.hops.append(Hop(tile, wide, steps, tiles))
            tile += wide
        spare = sum(max(0, hop.bottom - hop.top) for hop in self.hops[:-1])
        self.first_swap = max(self.n1, self.n0 - spare)
        left = self.first_swap
        for hop in self.hops[:-1]:
            take = max(0, min(self.n0 - left, hop.bottom - hop.top))
            hop.rest = (left, take)
            hop.swap = max(hop.bottom, hop.top + take)
            left += take


def split(x):
    high = x.astype(BF16)
    return high, (x - high.astype(F32)).astype(BF16)


def pick(row, values):
    result = values[0]
    for r, value in enumerate(values[1:], 1):
        result = jnp.where(row == r, value, result)
    return result


def own_kernel(plan, counts, pops, table, g_ref, ah, al, own0, own1, send, high, low):
    cohorts, people, span = g_ref.shape
    wide = span // TILE
    step = pl.program_id(0)
    group = lax.axis_index("pop")
    lane = lax.broadcasted_iota(jnp.int32, (1, TILE), 1)
    for w in range(wide):
        t = step * wide + w
        place = lax.axis_index("snp") * plan.tiles + t
        mask = (lane < counts[t]).astype(F32)
        total = table[pops[0], place]
        for e in range(1, pops.shape[0]):
            total = total + table[pops[e], place]
        rows = pl.ds(pl.multiple_of(t * TILE, TILE), TILE)
        columns = slice(w * TILE, (w + 1) * TILE)

        def prepare(i, carry):
            c, k = i // (people // STRIP), i % (people // STRIP)
            deep = pl.ds(pl.multiple_of(i * STRIP, STRIP), STRIP)
            x = g_ref[c, pl.ds(pl.multiple_of(k * STRIP, STRIP), STRIP), columns] * mask
            high[deep, columns], low[deep, columns] = split(x)
            share = table[pops[group * cohorts + c], place]
            coef = jnp.full((1, TILE), share, F32) / jnp.full((1, TILE), total, F32) * (1.0 / people)
            ah[rows, deep], al[rows, deep] = split((x * coef).T)
            return carry

        lax.fori_loop(0, cohorts * people // STRIP, prepare, 0)

    def block(q, carry):
        rows = pl.ds(pl.multiple_of(q * span, span), span)
        prod = jnp.dot(ah[rows, :], high[...], preferred_element_type=F32)
        prod = prod + jnp.dot(ah[rows, :], low[...], preferred_element_type=F32)
        prod = prod + jnp.dot(al[rows, :], high[...], preferred_element_type=F32)
        for k in range(wide):
            row = q * wide + k
            start = pick(row, plan.starts)
            for w in range(wide):
                m = step * wide + w - row
                spot = start + m
                inside = (m >= 0) & (m <= plan.steps)
                tile = prod[k * TILE : (k + 1) * TILE, w * TILE : (w + 1) * TILE]

                @pl.when(inside & (row < plan.half))
                def _():
                    own0[spot] = tile

                @pl.when(inside & (row >= plan.half))
                def _():
                    own1[spot] = tile

                @pl.when(inside & ((row < plan.half) == (group == 1)) & (spot < plan.first_swap))
                def _():
                    send[spot] = tile

        return carry

    lax.fori_loop(jnp.maximum(step * wide - plan.steps, 0) // wide, step + 1, block, 0)


def own_part(plan, genotypes, tile_counts, pop_id, weights):
    cohorts, people, snps = genotypes.shape
    deep = cohorts * people
    span = 2 * TILE
    tall = jax.ShapeDtypeStruct((snps, deep), BF16)
    sizes = (plan.n0, plan.n1, plan.first_swap)
    return pl.pallas_call(
        functools.partial(own_kernel, plan),
        grid=(snps // span,),
        in_specs=[SMEM, SMEM, SMEM, pl.BlockSpec((cohorts, people, span), lambda t: (0, 0, t))],
        out_specs=[VMEM] * 5,
        out_shape=[tall, tall] + [jax.ShapeDtypeStruct((n, TILE, TILE), F32) for n in sizes],
        scratch_shapes=[pltpu.VMEM((deep, span), BF16), pltpu.VMEM((deep, span), BF16)],
        cost_estimate=pl.CostEstimate(
            flops=6 * deep * snps * snps * 5 // 8, bytes_accessed=4 * deep * snps, transcendentals=0
        ),
        compiler_params=PARAMS,
    )(tile_counts, pop_id, weights, genotypes)


def hop_kernel(plan, hop, got, ah, al, *refs):
    refs = list(refs)
    own0 = refs.pop(0) if hop.rest[1] else None
    top = refs.pop(0) if hop.top else None
    bottom = refs.pop(0)
    low, high = refs.pop(), refs.pop()
    send = refs.pop() if refs else None
    group = lax.axis_index("pop")
    wide = hop.wide
    people = got.shape[1]

    def prepare(i, carry):
        c, k = i // (people // STRIP), i % (people // STRIP)
        deep = pl.ds(pl.multiple_of(i * STRIP, STRIP), STRIP)
        high[deep, :], low[deep, :] = split(got[c, pl.ds(pl.multiple_of(k * STRIP, STRIP), STRIP), :])
        return carry

    lax.fori_loop(0, got.shape[0] * people // STRIP, prepare, 0)

    def block(row, tall):
        rows = pl.ds(pl.multiple_of(row * TILE, TILE), tall * TILE)
        if wide == 1:
            both = jnp.concatenate([high[...], low[...]], axis=1)
            prod = jnp.dot(ah[rows, :], both, preferred_element_type=F32)
            prod = prod[:, :TILE] + prod[:, TILE:]
        else:
            prod = jnp.dot(ah[rows, :], high[...], preferred_element_type=F32)
            prod = prod + jnp.dot(ah[rows, :], low[...], preferred_element_type=F32)
        prod = prod + jnp.dot(al[rows, :], high[...], preferred_element_type=F32)
        for k in range(tall):

            def put(out, base, owner):
                for w in range(wide):
                    tile = prod[k * TILE : (k + 1) * TILE, w * TILE : (w + 1) * TILE]
                    spot = (row + k - base) * wide + w
                    out[spot] = tile
                    if send is not None:

                        @pl.when(group == owner)
                        def _():
                            send[spot] = tile

            if top is not None:
                upper = (row + k >= hop.first) & (row + k < plan.half)
                pl.when(upper)(functools.partial(put, top, hop.first, 1))
            pl.when(row + k >= hop.base)(functools.partial(put, bottom, hop.base, 0))

    even = hop.first // 2

    def pair(q, carry):
        block(2 * q, 2)
        return carry

    if plan.tiles - hop.first > 1:
        lax.fori_loop(even, plan.tiles // 2, pair, 0)
    else:
        block(hop.first, 1)
    if hop.rest[1]:

        @pl.when(group == 1)
        def _():
            send[hop.top : hop.top + hop.rest[1]] = own0[hop.rest[0] : hop.rest[0] + hop.rest[1]]


def hop_part(plan, hop, got, ah, al, own0, tag):
    deep = ah.shape[1]
    span = hop.wide * TILE
    args = [got, ah, al] + ([own0] if hop.rest[1] else [])
    sizes = ([hop.top] if hop.top else []) + [hop.bottom] + ([hop.swap] if tag + 1 < len(plan.hops) else [])
    outs = pl.pallas_call(
        functools.partial(hop_kernel, plan, hop),
        in_specs=[VMEM] * len(args),
        out_specs=[VMEM] * len(sizes),
        out_shape=[jax.ShapeDtypeStruct((n, TILE, TILE), F32) for n in sizes],
        scratch_shapes=[pltpu.VMEM((deep, span), BF16), pltpu.VMEM((deep, span), BF16)],
        cost_estimate=pl.CostEstimate(
            flops=6 * deep * span * (plan.tiles - hop.first) * TILE,
            bytes_accessed=4 * deep * span,
            transcendentals=0,
        ),
        compiler_params=PARAMS,
    )(*args)
    outs = list(outs)
    top = outs.pop(0) if hop.top else None
    return top, outs[0], outs[-1]


def skew(tile):
    groups = [tile[g : g + 8] for g in range(0, TILE, 8)]
    tile = jnp.concatenate([pltpu.roll(x, (TILE - 8 * g) % TILE, 1) if g else x for g, x in enumerate(groups)], axis=0)
    row = lax.broadcasted_iota(jnp.int32, (TILE, TILE), 0)
    for bit in (1, 2, 4):
        tile = jnp.where((row & bit) != 0, pltpu.roll(tile, TILE - bit, 1), tile)
    return tile


def band_tile(this, after, step, window):
    lane = lax.broadcasted_iota(jnp.int32, (TILE, TILE), 1)
    row = lax.broadcasted_iota(jnp.int32, (TILE, TILE), 0)
    mixed = jnp.where(lane + row < TILE, this, after)
    return jnp.where(step * TILE + lane < window, mixed, 0.0)


def runs(plan, h, r, own, swapped, parts):
    row = h * plan.half + r
    start, count = plan.starts[row], plan.counts[row]
    result = []
    edges = [(swapped, 0, plan.first_swap, 0)]
    if h == 0:
        edges += [(part[2], hop.rest[0], hop.rest[1], hop.top) for hop, part in zip(plan.hops, parts)]
    for came, begin, length, base in edges:
        lo, hi = max(start, begin), min(start + count, begin + length)
        if lo < hi:
            result.append((own[h], lo, came, base + lo - begin, lo - start, hi - lo))
    for hop, (top, bottom, came) in zip(plan.hops, parts):
        if row < hop.first:
            continue
        step = plan.tiles + hop.tile - row
        spot = (row - (hop.base if h else hop.first)) * hop.wide
        result.append((bottom if h else top, spot, came, spot, step, min(hop.wide, plan.steps + 1 - step)))
    return result


def finish_kernel(plan, window, own0, own1, swapped, *refs):
    refs = list(refs)
    band = refs.pop()
    out = refs.pop()
    parts = []
    for hop in plan.hops[:-1]:
        top = refs.pop(0) if hop.top else None
        parts.append((top, refs.pop(0), refs.pop(0)))
    group = lax.axis_index("pop")
    for h in range(2):

        @pl.when(group == h)
        def _():
            for r in range(plan.half):
                for kept, a, came, b, step, count in runs(plan, h, r, (own0, own1), swapped, parts):

                    def add(i, carry, r=r, kept=kept, a=a, came=came, b=b, step=step):
                        band[r, step + i] = kept[a + i] + came[b + i]
                        return carry

                    lax.fori_loop(0, count, add, 0)

    def line(r, carry):
        rows = pl.ds(pl.multiple_of(r * TILE, TILE), TILE)
        this = skew(band[r, 0])
        for m in range(plan.steps):
            after = skew(band[r, m + 1])
            out[rows, m * TILE : (m + 1) * TILE] = band_tile(this, after, m, window[0])
            this = after
        if plan.steps * TILE < out.shape[1]:
            out[rows, plan.steps * TILE :] = jnp.zeros((TILE, out.shape[1] - plan.steps * TILE), F32)
        return carry

    lax.fori_loop(0, plan.half, line, 0)


def last_kernel(plan, window, old, k0, k1, c0, c1, out):
    this = skew(k0[k0.shape[0] - 1] + c0[plan.hops[-2].bottom - 1])
    after = skew(k1[0] + c1[0])
    fresh = band_tile(this, after, plan.steps - 1, window[0])
    out[...] = jnp.where(lax.axis_index("pop") == 1, fresh, old[...])


def band(steps, genotypes, pop_id, window, tile_counts, weights):
    snps = genotypes.shape[2]
    tiles = snps // TILE
    half = tiles // 2
    assert snps == WIN and tiles % 2 == 0 and lax.axis_size("pop") == 2
    plan = Plan(steps, tiles)
    valid = (tile_counts[:, None] > jnp.arange(TILE, dtype=jnp.int32)[None, :]).astype(F32).reshape(snps)
    behind = [(i + 1, i) for i in range(lax.axis_size("snp") - 1)]

    def swap(block, route):
        return lax.ppermute(block, "pop", route)

    arrivals = []
    for j, hop in enumerate(plan.hops):
        if j == 2:
            ah, al, own0, own1, send = own_part(plan, genotypes, tile_counts, pop_id, weights)
            valid, send, piece = lax.optimization_barrier((valid, send, piece))
        elif j:
            valid, piece = lax.optimization_barrier((valid, piece))
        span = slice(hop.tile * TILE, (hop.tile + hop.wide) * TILE)
        piece = genotypes[:, :, span] * valid[span]
        arrivals.append(lax.ppermute(piece, "snp", behind))
    both = [(0, 1), (1, 0)]
    swapped = swap(send, both)
    parts = []
    for j, (hop, got) in enumerate(zip(plan.hops, arrivals)):
        top, bottom, send = hop_part(plan, hop, got, ah, al, own0, j)
        route = both if hop.top or hop.rest[1] else both[:1]
        parts.append((top, bottom, swap(send, route)))
    lists = [own0, own1, swapped]
    for part in parts[:-1]:
        lists += [x for x in part if x is not None]
    shape = jax.ShapeDtypeStruct((half * TILE, WIN), F32)
    finish = pl.pallas_call(
        functools.partial(finish_kernel, plan),
        in_specs=[SMEM] + [VMEM] * len(lists),
        out_specs=VMEM,
        out_shape=shape,
        scratch_shapes=[pltpu.VMEM((half, steps + 1, TILE, TILE), F32)],
        cost_estimate=pl.CostEstimate(flops=10**9, bytes_accessed=6 * half * TILE * WIN * 4, transcendentals=0),
        compiler_params=PARAMS,
    )
    out = finish(window, *lists)
    corner = pl.BlockSpec((TILE, TILE), lambda i: (half - 1, steps - 1))
    return pl.pallas_call(
        functools.partial(last_kernel, plan),
        grid=(1,),
        in_specs=[SMEM, corner, VMEM, VMEM, VMEM, VMEM],
        out_specs=corner,
        out_shape=shape,
        input_output_aliases={1: 0},
        cost_estimate=pl.CostEstimate(flops=10**7, bytes_accessed=6 * TILE * TILE * 4, transcendentals=0),
        compiler_params=PARAMS,
    )(window, out, parts[-2][1], parts[-1][1], parts[-2][2], parts[-1][2])


def solution(mesh):
    sizes = sorted(HOPS)

    def branch(steps):
        def body(*args):
            return band(steps, *args)

        return body

    def body(genotypes, pop_id, window, tile_counts, weights):
        steps = (window[0] + TILE - 1) // TILE
        return lax.switch(
            jnp.clip(steps - sizes[0], 0, len(sizes) - 1),
            [branch(n) for n in sizes],
            genotypes,
            pop_id,
            window,
            tile_counts,
            weights,
        )

    return jax.shard_map(
        body,
        mesh=mesh,
        in_specs=(P("pop", None, "snp"), P(), P(), P("snp"), P()),
        out_specs=P(("snp", "pop"), None),
        check_vma=False,
    )
```

```python
import functools

import jax
import jax.numpy as jnp
from jax import lax
from jax.experimental import pallas as pl
from jax.experimental.pallas import tpu as pltpu
from jax.sharding import PartitionSpec as P


WIN = 1024
TILE = 128
STRIP = 256
OWN_STRIP = 1024
F32 = jnp.float32
BF16 = jnp.bfloat16
SMEM = pl.BlockSpec(memory_space=pltpu.SMEM)
VMEM = pl.BlockSpec(memory_space=pltpu.VMEM)
PARAMS = pltpu.CompilerParams(vmem_limit_bytes=20 * 2**20)
HOPS = {8: (2, 2, 2, 1, 1), 7: (2, 2, 2, 1), 6: (2, 2, 1, 1), 5: (2, 2, 1)}


class Hop:
    def __init__(self, tile, wide, steps, tiles):
        self.tile, self.wide = tile, wide
        self.first = tile + tiles - steps
        self.base = max(self.first, tiles // 2)
        self.top = max(0, tiles // 2 - self.first) * wide
        self.bottom = (tiles - self.base) * wide
        self.rest = (0, 0)


class Plan:
    def __init__(self, steps, tiles):
        self.steps, self.tiles, self.half = steps, tiles, tiles // 2
        self.counts = [min(steps + 1, tiles - r) for r in range(tiles)]
        starts = [sum(self.counts[:r]) for r in range(tiles + 1)]
        self.n0 = starts[self.half]
        self.n1 = starts[tiles] - self.n0
        self.starts = [s if r < self.half else s - self.n0 for r, s in enumerate(starts[:tiles])]
        self.hops, tile = [], 0
        for wide in HOPS[steps]:
            self.hops.append(Hop(tile, wide, steps, tiles))
            tile += wide
        assert self.hops[-2].first >= self.half
        spare = sum(max(0, hop.bottom - hop.top) for hop in self.hops[:-2])
        self.first_swap = max(self.n1, self.n0 - spare)
        left = self.first_swap
        for hop in self.hops[:-2]:
            take = max(0, min(self.n0 - left, hop.bottom - hop.top))
            hop.rest = (left, take)
            hop.swap = max(hop.bottom, hop.top + take)
            left += take
        assert left == self.n0 or left == self.first_swap > self.n0


def split(x):
    high = x.astype(BF16)
    return high, (x - high.astype(F32)).astype(BF16)


def pick(row, values):
    result = values[0]
    for r, value in enumerate(values[1:], 1):
        result = jnp.where(row == r, value, result)
    return result


def own_kernel(plan, counts, pops, table, g_ref, ah, al, own0, own1, send, high, low):
    cohorts, people, span = g_ref.shape
    wide = span // TILE
    step = pl.program_id(0)
    group = lax.axis_index("pop")
    lane = lax.broadcasted_iota(jnp.int32, (1, TILE), 1)
    for w in range(wide):
        t = step * wide + w
        place = lax.axis_index("snp") * plan.tiles + t
        mask = (lane < counts[t]).astype(F32)
        total = table[pops[0], place]
        for e in range(1, pops.shape[0]):
            total = total + table[pops[e], place]
        rows = pl.ds(pl.multiple_of(t * TILE, TILE), TILE)
        columns = slice(w * TILE, (w + 1) * TILE)

        def prepare(i, carry):
            c, k = i // (people // OWN_STRIP), i % (people // OWN_STRIP)
            deep = pl.ds(pl.multiple_of(i * OWN_STRIP, OWN_STRIP), OWN_STRIP)
            x = g_ref[c, pl.ds(pl.multiple_of(k * OWN_STRIP, OWN_STRIP), OWN_STRIP), columns] * mask
            high[deep, columns], low[deep, columns] = split(x)
            share = table[pops[group * cohorts + c], place]
            coef = jnp.full((1, TILE), share, F32) / jnp.full((1, TILE), total, F32) * (1.0 / people)
            ah[rows, deep], al[rows, deep] = split((x * coef).T)
            return carry

        lax.fori_loop(0, cohorts * people // OWN_STRIP, prepare, 0)

    def block(q, carry):
        rows = pl.ds(pl.multiple_of(q * span, span), span)
        prod = jnp.dot(ah[rows, :], high[...], preferred_element_type=F32)
        prod = prod + jnp.dot(ah[rows, :], low[...], preferred_element_type=F32)
        prod = prod + jnp.dot(al[rows, :], high[...], preferred_element_type=F32)
        for k in range(wide):
            row = q * wide + k
            start = pick(row, plan.starts)
            for w in range(wide):
                m = step * wide + w - row
                spot = start + m
                inside = (m >= 0) & (m <= plan.steps)
                tile = prod[k * TILE : (k + 1) * TILE, w * TILE : (w + 1) * TILE]

                @pl.when(inside & (row < plan.half))
                def _():
                    own0[spot] = tile

                @pl.when(inside & (row >= plan.half))
                def _():
                    own1[spot] = tile

                @pl.when(inside & ((row < plan.half) == (group == 1)) & (spot < plan.first_swap))
                def _():
                    send[spot] = tile

        return carry

    lax.fori_loop(jnp.maximum(step * wide - plan.steps, 0) // wide, step + 1, block, 0)


def own_part(plan, genotypes, tile_counts, pop_id, weights):
    cohorts, people, snps = genotypes.shape
    deep = cohorts * people
    span = 2 * TILE
    tall = jax.ShapeDtypeStruct((snps, deep), BF16)
    sizes = (plan.n0, plan.n1, plan.first_swap)
    return pl.pallas_call(
        functools.partial(own_kernel, plan),
        grid=(snps // span,),
        in_specs=[SMEM, SMEM, SMEM, pl.BlockSpec((cohorts, people, span), lambda t: (0, 0, t))],
        out_specs=[VMEM] * 5,
        out_shape=[tall, tall] + [jax.ShapeDtypeStruct((n, TILE, TILE), F32) for n in sizes],
        scratch_shapes=[pltpu.VMEM((deep, span), BF16), pltpu.VMEM((deep, span), BF16)],
        cost_estimate=pl.CostEstimate(
            flops=6 * deep * snps * snps * 5 // 8, bytes_accessed=4 * deep * snps, transcendentals=0
        ),
        compiler_params=PARAMS,
    )(tile_counts, pop_id, weights, genotypes)


def hop_kernel(plan, hop, got, ah, al, *refs):
    refs = list(refs)
    own0 = refs.pop(0) if hop.rest[1] else None
    top = refs.pop(0) if hop.top else None
    bottom = refs.pop(0)
    low, high = refs.pop(), refs.pop()
    send = refs.pop() if refs else None
    group = lax.axis_index("pop")
    wide = hop.wide
    people = got.shape[1]

    def prepare(i, carry):
        c, k = i // (people // STRIP), i % (people // STRIP)
        deep = pl.ds(pl.multiple_of(i * STRIP, STRIP), STRIP)
        high[deep, :], low[deep, :] = split(got[c, pl.ds(pl.multiple_of(k * STRIP, STRIP), STRIP), :])
        return carry

    lax.fori_loop(0, got.shape[0] * people // STRIP, prepare, 0)

    def block(row, tall):
        rows = pl.ds(pl.multiple_of(row * TILE, TILE), tall * TILE)
        if wide == 1:
            both = jnp.concatenate([high[...], low[...]], axis=1)
            prod = jnp.dot(ah[rows, :], both, preferred_element_type=F32)
            prod = prod[:, :TILE] + prod[:, TILE:]
        else:
            prod = jnp.dot(ah[rows, :], high[...], preferred_element_type=F32)
            prod = prod + jnp.dot(ah[rows, :], low[...], preferred_element_type=F32)
        prod = prod + jnp.dot(al[rows, :], high[...], preferred_element_type=F32)
        for k in range(tall):

            def put(out, base, owner):
                for w in range(wide):
                    tile = prod[k * TILE : (k + 1) * TILE, w * TILE : (w + 1) * TILE]
                    spot = (row + k - base) * wide + w
                    out[spot] = tile
                    if send is not None:

                        @pl.when(group == owner)
                        def _():
                            send[spot] = tile

            if top is not None:
                upper = (row + k >= hop.first) & (row + k < plan.half)
                pl.when(upper)(functools.partial(put, top, hop.first, 1))
            pl.when(row + k >= hop.base)(functools.partial(put, bottom, hop.base, 0))

    even = hop.first // 2

    def pair(q, carry):
        block(2 * q, 2)
        return carry

    if plan.tiles - hop.first > 1:
        lax.fori_loop(even, plan.tiles // 2, pair, 0)
    else:
        block(hop.first, 1)
    if hop.rest[1]:

        @pl.when(group == 1)
        def _():
            send[hop.top : hop.top + hop.rest[1]] = own0[hop.rest[0] : hop.rest[0] + hop.rest[1]]


def hop_part(plan, hop, got, ah, al, own0, tag):
    deep = ah.shape[1]
    span = hop.wide * TILE
    args = [got, ah, al] + ([own0] if hop.rest[1] else [])
    sizes = ([hop.top] if hop.top else []) + [hop.bottom] + ([hop.swap] if tag + 2 < len(plan.hops) else [])
    outs = pl.pallas_call(
        functools.partial(hop_kernel, plan, hop),
        in_specs=[VMEM] * len(args),
        out_specs=[VMEM] * len(sizes),
        out_shape=[jax.ShapeDtypeStruct((n, TILE, TILE), F32) for n in sizes],
        scratch_shapes=[pltpu.VMEM((deep, span), BF16), pltpu.VMEM((deep, span), BF16)],
        cost_estimate=pl.CostEstimate(
            flops=6 * deep * span * (plan.tiles - hop.first) * TILE,
            bytes_accessed=4 * deep * span,
            transcendentals=0,
        ),
        compiler_params=PARAMS,
    )(*args)
    outs = list(outs)
    top = outs.pop(0) if hop.top else None
    return top, outs[0], outs[-1]


def skew(tiles, group):
    rows = tiles[0].shape[0]
    result = []
    for tile in tiles:
        parts = []
        for g in range(rows // 8):
            shift = (TILE - 8 * g - group * 8) % TILE
            parts.append(pltpu.roll(tile[8 * g : 8 * g + 8], shift, 1))
        result.append(jnp.concatenate(parts, axis=0))
    row = lax.broadcasted_iota(jnp.int32, (rows, TILE), 0)
    for bit in (1, 2, 4):
        odd = (row & bit) != 0
        result = [jnp.where(odd, pltpu.roll(tile, TILE - bit, 1), tile) for tile in result]
    return result


def band_tiles(tiles, first, group, window):
    shape = tiles[0].shape
    lane = lax.broadcasted_iota(jnp.int32, shape, 1)
    near = lane + lax.broadcasted_iota(jnp.int32, shape, 0) + group * 8 < TILE
    for m, (this, after) in enumerate(zip(tiles, tiles[1:]), first):
        yield jnp.where(m * TILE + lane < window, jnp.where(near, this, after), 0.0)


def runs(plan, h, r, own, swapped, parts):
    row = h * plan.half + r
    start, count = plan.starts[row], plan.counts[row]
    result = []
    edges = [(swapped, 0, plan.first_swap, 0)]
    if h == 0:
        edges += [(part[2], hop.rest[0], hop.rest[1], hop.top) for hop, part in zip(plan.hops, parts)]
    for came, begin, length, base in edges:
        lo, hi = max(start, begin), min(start + count, begin + length)
        if lo < hi:
            result.append((own[h], lo, came, base + lo - begin, lo - start, hi - lo))
    for hop, (top, bottom, came) in zip(plan.hops, parts):
        if row < hop.first:
            continue
        step = plan.tiles + hop.tile - row
        spot = (row - (hop.base if h else hop.first)) * hop.wide
        result.append((bottom if h else top, spot, came, spot, step, min(hop.wide, plan.steps + 1 - step)))
    return result


def finish_kernel(plan, window, own0, own1, swapped, *refs):
    refs = list(refs)
    sems, lines, band, edge, out = (refs.pop() for _ in range(5))
    parts = []
    for hop in plan.hops[:-2]:
        top = refs.pop(0) if hop.top else None
        parts.append((top, refs.pop(0), refs.pop(0)))
    group = lax.axis_index("pop")
    for h in range(2):

        @pl.when(group == h)
        def _():
            for r in range(plan.half):
                for kept, a, came, b, step, count in runs(plan, h, r, (own0, own1), swapped, parts):

                    def add(i, carry, r=r, kept=kept, a=a, came=came, b=b, step=step):
                        band[r, step + i] = kept[a + i] + came[b + i]
                        return carry

                    lax.fori_loop(0, count, add, 0)

    for i in range(edge.shape[0]):
        row = plan.hops[-2].first + i
        edge[i] = band[row - plan.half, plan.tiles + plan.hops[-2].tile - row - 1]

    strip = 32
    strips = TILE // strip

    def line(i, carry):
        r, q = i // strips, i % strips
        inner = pl.ds(pl.multiple_of(q * strip, strip), strip)
        rows = pl.ds(pl.multiple_of(i * strip, strip), strip)
        tiles = skew([band[r, m, inner, :] for m in range(plan.steps + 1)], q * (strip // 8))
        for m, tile in enumerate(band_tiles(tiles, 0, q * (strip // 8), window[0])):
            lines[rows, m * TILE : (m + 1) * TILE] = tile
        if plan.steps * TILE < out.shape[1]:
            lines[rows, plan.steps * TILE :] = jnp.zeros((strip, out.shape[1] - plan.steps * TILE), F32)

        @pl.when(q == strips - 1)
        def _():
            leave(r).start()

        return carry

    def leave(r):
        rows = pl.ds(pl.multiple_of(r * TILE, TILE), TILE)
        return pltpu.make_async_copy(lines.at[rows, :], out.at[rows, :], sems.at[r])

    lax.fori_loop(0, plan.half * strips, line, 0)
    for r in range(plan.half):
        leave(r).wait()


def last_kernel(plan, window, old, edge, kept, came, kept_last, came_last, out, fresh, sems):
    del old
    hop, final = plan.hops[-2:]

    @pl.when(lax.axis_index("pop") == 1)
    def _():
        copies = []
        for i in range(edge.shape[0]):
            row = hop.first + i
            step = plan.tiles + hop.tile - row
            tiles = [edge[i]]
            for w in range(min(hop.wide, plan.steps + 1 - step)):
                tiles.append(kept[i * hop.wide + w] + came[i * hop.wide + w])
            if row >= final.first:
                tiles.append(kept_last[row - final.first] + came_last[row - final.first])
            for m, tile in enumerate(band_tiles(skew(tiles, 0), step - 1, 0, window[0])):
                fresh[i, :, m * TILE : (m + 1) * TILE] = tile
            width = (plan.steps - step + 1) * TILE
            copies.append(
                pltpu.make_async_copy(
                    fresh.at[i, :, pl.ds(0, width)],
                    out.at[pl.ds((row - plan.half) * TILE, TILE), pl.ds((step - 1) * TILE, width)],
                    sems.at[i],
                )
            )
            copies[-1].start()
        for copy in copies:
            copy.wait()


def band(steps, genotypes, pop_id, window, tile_counts, weights):
    snps = genotypes.shape[2]
    tiles = snps // TILE
    half = tiles // 2
    assert snps == WIN and tiles % 2 == 0 and lax.axis_size("pop") == 2
    plan = Plan(steps, tiles)
    valid = (tile_counts[:, None] > jnp.arange(TILE, dtype=jnp.int32)[None, :]).astype(F32).reshape(snps)
    behind = [(i + 1, i) for i in range(lax.axis_size("snp") - 1)]

    def swap(block, route):
        return lax.ppermute(block, "pop", route)

    both = [(0, 1), (1, 0)]
    arrivals = []
    for j, hop in enumerate(plan.hops):
        span = slice(hop.tile * TILE, (hop.tile + hop.wide) * TILE)
        piece = genotypes[:, :, span] * valid[span]
        arrivals.append(lax.ppermute(piece, "snp", behind))
        if j == 0:
            ah, al, own0, own1, send = own_part(plan, genotypes, tile_counts, pop_id, weights)
            swapped = swap(send, both)
            valid, send, piece = lax.optimization_barrier((valid, send, piece))
        else:
            valid, piece = lax.optimization_barrier((valid, piece))
    parts = []
    for j, (hop, got) in enumerate(zip(plan.hops, arrivals)):
        top, bottom, send = hop_part(plan, hop, got, ah, al, own0, j)
        route = both if hop.top or hop.rest[1] else both[:1]
        parts.append((top, bottom, swap(send, route)))
    lists = [own0, own1, swapped]
    for part in parts[:-2]:
        lists += [x for x in part if x is not None]
    shape = jax.ShapeDtypeStruct((half * TILE, WIN), F32)
    anywhere = pl.BlockSpec(memory_space=pl.ANY)
    open_rows = tiles - plan.hops[-2].first
    finish = pl.pallas_call(
        functools.partial(finish_kernel, plan),
        in_specs=[SMEM] + [VMEM] * len(lists),
        out_specs=[anywhere, VMEM],
        out_shape=[shape, jax.ShapeDtypeStruct((open_rows, TILE, TILE), F32)],
        scratch_shapes=[
            pltpu.VMEM((half, steps + 1, TILE, TILE), F32),
            pltpu.VMEM((half * TILE, WIN), F32),
            pltpu.SemaphoreType.DMA((half,)),
        ],
        cost_estimate=pl.CostEstimate(flops=10**9, bytes_accessed=6 * half * TILE * WIN * 4, transcendentals=0),
        compiler_params=PARAMS,
    )
    out, edge = finish(window, *lists)
    return pl.pallas_call(
        functools.partial(last_kernel, plan),
        in_specs=[SMEM, anywhere] + [VMEM] * 5,
        out_specs=anywhere,
        out_shape=shape,
        input_output_aliases={1: 0},
        scratch_shapes=[
            pltpu.VMEM((open_rows, TILE, (plan.hops[-2].wide + 1) * TILE), F32),
            pltpu.SemaphoreType.DMA((open_rows,)),
        ],
        cost_estimate=pl.CostEstimate(flops=10**7, bytes_accessed=6 * TILE * TILE * 4, transcendentals=0),
        compiler_params=PARAMS,
    )(window, out, edge, parts[-2][1], parts[-2][2], parts[-1][1], parts[-1][2])


def solution(mesh):
    sizes = sorted(HOPS)

    def branch(steps):
        def body(*args):
            return band(steps, *args)

        return body

    def body(genotypes, pop_id, window, tile_counts, weights):
        steps = (window[0] + TILE - 1) // TILE
        return lax.switch(
            jnp.clip(steps - sizes[0], 0, len(sizes) - 1),
            [branch(n) for n in sizes],
            genotypes,
            pop_id,
            window,
            tile_counts,
            weights,
        )

    return jax.shard_map(
        body,
        mesh=mesh,
        in_specs=(P("pop", None, "snp"), P(), P(), P("snp"), P()),
        out_specs=P(("snp", "pop"), None),
        check_vma=False,
    )
```

```python
import functools

import jax
import jax.numpy as jnp
from jax import lax
from jax.experimental import pallas as pl
from jax.experimental.pallas import tpu as pltpu
from jax.sharding import PartitionSpec as P


WIN = 1024
TILE = 128
STRIP = 256
OWN_STRIP = 512
F32 = jnp.float32
BF16 = jnp.bfloat16
SMEM = pl.BlockSpec(memory_space=pltpu.SMEM)
VMEM = pl.BlockSpec(memory_space=pltpu.VMEM)
PARAMS = pltpu.CompilerParams(vmem_limit_bytes=20 * 2**20)
HOPS = {8: (2, 2, 2, 1, 1), 7: (2, 2, 2, 1), 6: (2, 2, 1, 1), 5: (2, 2, 1)}


class Hop:
    def __init__(self, tile, wide, steps, tiles):
        self.tile, self.wide = tile, wide
        self.first = tile + tiles - steps
        self.base = max(self.first, tiles // 2)
        self.top = max(0, tiles // 2 - self.first) * wide
        self.bottom = (tiles - self.base) * wide
        self.rest = (0, 0)


class Plan:
    def __init__(self, steps, tiles):
        self.steps, self.tiles, self.half = steps, tiles, tiles // 2
        self.counts = [min(steps + 1, tiles - r) for r in range(tiles)]
        starts = [sum(self.counts[:r]) for r in range(tiles + 1)]
        self.n0 = starts[self.half]
        self.n1 = starts[tiles] - self.n0
        self.starts = [s if r < self.half else s - self.n0 for r, s in enumerate(starts[:tiles])]
        self.hops, tile = [], 0
        for wide in HOPS[steps]:
            self.hops.append(Hop(tile, wide, steps, tiles))
            tile += wide
        assert self.hops[-2].first >= self.half
        assert self.hops[-1].first == tiles - 1 and self.hops[-1].wide == 1
        spare = sum(max(0, hop.bottom - hop.top) for hop in self.hops[:-2])
        self.first_swap = max(self.n1, self.n0 - spare)
        self.even = self.n1 if steps == min(HOPS) else self.first_swap
        self.extra = self.first_swap - self.even
        left = self.first_swap
        for hop in self.hops[:-2]:
            take = max(0, min(self.n0 - left, hop.bottom - hop.top))
            hop.rest = (left, take)
            hop.swap = max(hop.bottom, hop.top + take)
            left += take
        assert left == self.n0 or left == self.first_swap > self.n0


def split(x):
    high = x.astype(BF16)
    return high, (x - high.astype(F32)).astype(BF16)


def pick(row, values):
    result = values[0]
    for r, value in enumerate(values[1:], 1):
        result = jnp.where(row == r, value, result)
    return result


def piece_kernel(counts_ref, g_ref, out, counts, sems):
    cohorts, people, span = out.shape
    parts = (sems.shape[0] - 1) // cohorts
    rows = people // parts
    copies = []
    for i in range(cohorts * parts):
        c, k = i // parts, i % parts
        area = (c, pl.ds(k * rows, rows))
        copies.append(
            pltpu.make_async_copy(g_ref.at[area + (pl.ds(0, span),)], out.at[area], sems.at[i])
        )
        copies[-1].start()
    table = pltpu.make_async_copy(counts_ref, counts, sems.at[cohorts * parts])
    table.start()
    table.wait()
    lane = lax.broadcasted_iota(jnp.int32, (1, TILE), 1)
    mask = jnp.concatenate([(lane < counts[w]).astype(F32) for w in range(span // TILE)], axis=1)
    for i, copy in enumerate(copies):
        copy.wait()
        c, k = i // parts, i % parts

        def cut(j, carry, c=c, k=k):
            area = pl.ds(pl.multiple_of(k * rows + j * 128, 128), 128)
            out[c, area, :] = out[c, area, :] * mask
            return carry

        lax.fori_loop(0, rows // 128, cut, 0)


def piece_part(genotypes, tile_counts, wide):
    cohorts, people, _ = genotypes.shape
    return pl.pallas_call(
        piece_kernel,
        in_specs=[pl.BlockSpec(memory_space=pl.ANY)] * 2,
        out_specs=VMEM,
        out_shape=jax.ShapeDtypeStruct((cohorts, people, wide * TILE), F32),
        scratch_shapes=[pltpu.SMEM(tile_counts.shape, jnp.int32), pltpu.SemaphoreType.DMA((cohorts * 4 + 1,))],
        cost_estimate=pl.CostEstimate(flops=10**6, bytes_accessed=8 * cohorts * people * wide * TILE, transcendentals=0),
        compiler_params=PARAMS,
        name="piece",
    )(tile_counts, genotypes)


def own_kernel(plan, counts, pops, table, g_ref, ah, al, own0, own1, send, *refs):
    more = refs[0] if plan.extra else None
    high, low = refs[-2:]
    cohorts, people, span = g_ref.shape
    wide = span // TILE
    step = pl.program_id(0)
    group = lax.axis_index("pop")
    lane = lax.broadcasted_iota(jnp.int32, (1, TILE), 1)
    for w in range(wide):
        t = step * wide + w
        place = lax.axis_index("snp") * plan.tiles + t
        mask = (lane < counts[t]).astype(F32)
        total = table[pops[0], place]
        for e in range(1, pops.shape[0]):
            total = total + table[pops[e], place]
        rows = pl.ds(pl.multiple_of(t * TILE, TILE), TILE)
        columns = slice(w * TILE, (w + 1) * TILE)

        def prepare(i, carry):
            c, k = i // (people // OWN_STRIP), i % (people // OWN_STRIP)
            deep = pl.ds(pl.multiple_of(i * OWN_STRIP, OWN_STRIP), OWN_STRIP)
            x = g_ref[c, pl.ds(pl.multiple_of(k * OWN_STRIP, OWN_STRIP), OWN_STRIP), columns] * mask
            high[deep, columns], low[deep, columns] = split(x)
            share = table[pops[group * cohorts + c], place]
            coef = jnp.full((1, TILE), share, F32) / jnp.full((1, TILE), total, F32) * (1.0 / people)
            ah[rows, deep], al[rows, deep] = split((x * coef).T)
            return carry

        lax.fori_loop(0, cohorts * people // OWN_STRIP, prepare, 0)

    def block(q, carry):
        rows = pl.ds(pl.multiple_of(q * span, span), span)
        prod = jnp.dot(ah[rows, :], high[...], preferred_element_type=F32)
        prod = prod + jnp.dot(ah[rows, :], low[...], preferred_element_type=F32)
        prod = prod + jnp.dot(al[rows, :], high[...], preferred_element_type=F32)
        for k in range(wide):
            row = q * wide + k
            start = pick(row, plan.starts)
            for w in range(wide):
                m = step * wide + w - row
                spot = start + m
                inside = (m >= 0) & (m <= plan.steps)
                tile = prod[k * TILE : (k + 1) * TILE, w * TILE : (w + 1) * TILE]

                @pl.when(inside & (row < plan.half))
                def _():
                    own0[spot] = tile

                @pl.when(inside & (row >= plan.half))
                def _():
                    own1[spot] = tile

                other = inside & ((row < plan.half) == (group == 1))

                @pl.when(other & (spot < plan.even))
                def _():
                    send[spot] = tile

                if more is not None:

                    @pl.when(other & (spot >= plan.even) & (spot < plan.first_swap))
                    def _():
                        more[spot - plan.even] = tile

        return carry

    lax.fori_loop(jnp.maximum(step * wide - plan.steps, 0) // wide, step + 1, block, 0)


def own_part(plan, genotypes, tile_counts, pop_id, weights):
    cohorts, people, snps = genotypes.shape
    deep = cohorts * people
    span = 2 * TILE
    tall = jax.ShapeDtypeStruct((snps, deep), BF16)
    sizes = [plan.n0, plan.n1, plan.even] + ([plan.extra] if plan.extra else [])
    return pl.pallas_call(
        functools.partial(own_kernel, plan),
        grid=(snps // span,),
        in_specs=[SMEM, SMEM, SMEM, pl.BlockSpec((cohorts, people, span), lambda t: (0, 0, t))],
        out_specs=[VMEM] * (2 + len(sizes)),
        out_shape=[tall, tall] + [jax.ShapeDtypeStruct((n, TILE, TILE), F32) for n in sizes],
        scratch_shapes=[pltpu.VMEM((deep, span), BF16), pltpu.VMEM((deep, span), BF16)],
        cost_estimate=pl.CostEstimate(
            flops=6 * deep * snps * snps * 5 // 8, bytes_accessed=4 * deep * snps, transcendentals=0
        ),
        compiler_params=PARAMS,
    )(tile_counts, pop_id, weights, genotypes)


def hop_kernel(plan, hop, got, ah, al, *refs):
    refs = list(refs)
    own0 = refs.pop(0) if hop.rest[1] else None
    top = refs.pop(0) if hop.top else None
    bottom = refs.pop(0)
    low, high = refs.pop(), refs.pop()
    send = refs.pop() if refs else None
    group = lax.axis_index("pop")
    wide = hop.wide
    people = got.shape[1]

    def prepare(i, carry):
        c, k = i // (people // STRIP), i % (people // STRIP)
        deep = pl.ds(pl.multiple_of(i * STRIP, STRIP), STRIP)
        high[deep, :], low[deep, :] = split(got[c, pl.ds(pl.multiple_of(k * STRIP, STRIP), STRIP), :])
        return carry

    lax.fori_loop(0, got.shape[0] * people // STRIP, prepare, 0)

    def block(row, tall):
        rows = pl.ds(pl.multiple_of(row * TILE, TILE), tall * TILE)
        if wide == 1:
            both = jnp.concatenate([high[...], low[...]], axis=1)
            prod = jnp.dot(ah[rows, :], both, preferred_element_type=F32)
            prod = prod[:, :TILE] + prod[:, TILE:]
        else:
            prod = jnp.dot(ah[rows, :], high[...], preferred_element_type=F32)
            prod = prod + jnp.dot(ah[rows, :], low[...], preferred_element_type=F32)
        prod = prod + jnp.dot(al[rows, :], high[...], preferred_element_type=F32)
        for k in range(tall):

            def put(out, base, owner):
                for w in range(wide):
                    tile = prod[k * TILE : (k + 1) * TILE, w * TILE : (w + 1) * TILE]
                    spot = (row + k - base) * wide + w
                    out[spot] = tile
                    if send is not None:

                        @pl.when(group == owner)
                        def _():
                            send[spot] = tile

            if top is not None:
                upper = (row + k >= hop.first) & (row + k < plan.half)
                pl.when(upper)(functools.partial(put, top, hop.first, 1))
            pl.when(row + k >= hop.base)(functools.partial(put, bottom, hop.base, 0))

    even = hop.first // 2

    def pair(q, carry):
        block(2 * q, 2)
        return carry

    if plan.tiles - hop.first > 1:
        lax.fori_loop(even, plan.tiles // 2, pair, 0)
    else:
        block(hop.first, 1)
    if hop.rest[1]:

        @pl.when(group == 1)
        def _():
            send[hop.top : hop.top + hop.rest[1]] = own0[hop.rest[0] : hop.rest[0] + hop.rest[1]]


def hop_part(plan, hop, got, ah, al, own0, tag):
    deep = ah.shape[1]
    span = hop.wide * TILE
    args = [got, ah, al] + ([own0] if hop.rest[1] else [])
    sizes = ([hop.top] if hop.top else []) + [hop.bottom] + ([hop.swap] if tag + 2 < len(plan.hops) else [])
    outs = pl.pallas_call(
        functools.partial(hop_kernel, plan, hop),
        in_specs=[VMEM] * len(args),
        out_specs=[VMEM] * len(sizes),
        out_shape=[jax.ShapeDtypeStruct((n, TILE, TILE), F32) for n in sizes],
        scratch_shapes=[pltpu.VMEM((deep, span), BF16), pltpu.VMEM((deep, span), BF16)],
        cost_estimate=pl.CostEstimate(
            flops=6 * deep * span * (plan.tiles - hop.first) * TILE,
            bytes_accessed=4 * deep * span,
            transcendentals=0,
        ),
        compiler_params=PARAMS,
    )(*args)
    outs = list(outs)
    top = outs.pop(0) if hop.top else None
    return top, outs[0], outs[-1]


def skew(tiles, group):
    rows = tiles[0].shape[0]
    low = lax.broadcasted_iota(jnp.int32, (8, TILE), 0)
    row = lax.broadcasted_iota(jnp.int32, (rows, TILE), 0)
    result = []
    for tile in tiles:
        parts = []
        for g in range(rows // 8):
            part = tile[8 * g : 8 * g + 8]
            shift = 2 * TILE - 8 * g - group * 8
            near, far = pltpu.roll(part, shift % TILE, 1), pltpu.roll(part, (shift - 4) % TILE, 1)
            parts.append(jnp.where(low >= 4, far, near))
        result.append(jnp.concatenate(parts, axis=0))
    for bit in (1, 2):
        odd = (row & bit) != 0
        result = [jnp.where(odd, pltpu.roll(tile, TILE - bit, 1), tile) for tile in result]
    return result


def band_tiles(tiles, first, group, window):
    shape = tiles[0].shape
    lane = lax.broadcasted_iota(jnp.int32, shape, 1)
    near = lane + lax.broadcasted_iota(jnp.int32, shape, 0) + group * 8 < TILE
    for m, (this, after) in enumerate(zip(tiles, tiles[1:]), first):
        yield jnp.where(m * TILE + lane < window, jnp.where(near, this, after), 0.0)


def runs(plan, h, r, own, swapped, parts):
    row = h * plan.half + r
    start, count = plan.starts[row], plan.counts[row]
    result = []
    edges = [(swapped[0], 0, plan.even, 0)]
    if h == 0:
        edges += [(more, plan.even, plan.extra, 0) for more in swapped[1:]]
        edges += [(part[2], hop.rest[0], hop.rest[1], hop.top) for hop, part in zip(plan.hops, parts)]
    for came, begin, length, base in edges:
        lo, hi = max(start, begin), min(start + count, begin + length)
        if lo < hi:
            result.append((own[h], lo, came, base + lo - begin, lo - start, hi - lo))
    for hop, (top, bottom, came) in zip(plan.hops, parts):
        if row < hop.first:
            continue
        step = plan.tiles + hop.tile - row
        spot = (row - (hop.base if h else hop.first)) * hop.wide
        result.append((bottom if h else top, spot, came, spot, step, min(hop.wide, plan.steps + 1 - step)))
    return result


def finish_kernel(plan, window, own0, own1, *refs):
    refs = list(refs)
    swapped = [refs.pop(0) for _ in range(2 if plan.extra else 1)]
    sems, lines, band, edge, out = (refs.pop() for _ in range(5))
    parts = []
    for hop in plan.hops[:-2]:
        top = refs.pop(0) if hop.top else None
        parts.append((top, refs.pop(0), refs.pop(0)))
    group = lax.axis_index("pop")
    for h in range(2):

        @pl.when(group == h)
        def _():
            for r in range(plan.half):
                for kept, a, came, b, step, count in runs(plan, h, r, (own0, own1), swapped, parts):

                    def add(i, carry, r=r, kept=kept, a=a, came=came, b=b, step=step):
                        band[r, step + i] = kept[a + i] + came[b + i]
                        return carry

                    lax.fori_loop(0, count, add, 0)

    for i in range(edge.shape[0]):
        row = plan.hops[-2].first + i
        edge[i] = band[row - plan.half, plan.tiles + plan.hops[-2].tile - row - 1]

    strip = 64
    strips = TILE // strip

    def line(i, carry):
        r, q = i // strips, i % strips
        inner = pl.ds(pl.multiple_of(q * strip, strip), strip)
        rows = pl.ds(pl.multiple_of(i * strip, strip), strip)
        tiles = skew([band[r, m, inner, :] for m in range(plan.steps + 1)], q * (strip // 8))
        for m, tile in enumerate(band_tiles(tiles, 0, q * (strip // 8), window[0])):
            lines[rows, m * TILE : (m + 1) * TILE] = tile
        if plan.steps * TILE < out.shape[1]:
            lines[rows, plan.steps * TILE :] = jnp.zeros((strip, out.shape[1] - plan.steps * TILE), F32)
        leave(i).start()
        return carry

    def leave(i):
        rows = pl.ds(pl.multiple_of(i * strip, strip), strip)
        return pltpu.make_async_copy(lines.at[rows, :], out.at[rows, :], sems.at[i])

    lax.fori_loop(0, plan.half * strips, line, 0)
    for i in range(plan.half * strips):
        leave(i).wait()


def next_kernel(plan, window, old, edge, kept, came, out, ready, fresh, sems):
    del old
    hop = plan.hops[-2]

    @pl.when(lax.axis_index("pop") == 1)
    def _():
        copies = []
        for i in range(edge.shape[0]):
            row = hop.first + i
            step = plan.tiles + hop.tile - row
            tiles = [edge[i]]
            for w in range(min(hop.wide, plan.steps + 1 - step)):
                tiles.append(kept[i * hop.wide + w] + came[i * hop.wide + w])
            tiles = skew(tiles, 0)
            for m, tile in enumerate(band_tiles(tiles, step - 1, 0, window[0])):
                fresh[i, :, m * TILE : (m + 1) * TILE] = tile
            width = (len(tiles) - 1) * TILE
            copies.append(
                pltpu.make_async_copy(
                    fresh.at[i, :, pl.ds(0, width)],
                    out.at[pl.ds((row - plan.half) * TILE, TILE), pl.ds((step - 1) * TILE, width)],
                    sems.at[i],
                )
            )
            copies[-1].start()
        ready[0] = tiles[-1]
        for copy in copies:
            copy.wait()


def last_kernel(plan, window, old, ready, kept, came, out, fresh, sem):
    del old

    @pl.when(lax.axis_index("pop") == 1)
    def _():
        tiles = [ready[0]] + skew([kept[0] + came[0]], 0)
        (fresh[...],) = band_tiles(tiles, plan.steps - 1, 0, window[0])
        corner = out.at[pl.ds((plan.half - 1) * TILE, TILE), pl.ds((plan.steps - 1) * TILE, TILE)]
        copy = pltpu.make_async_copy(fresh, corner, sem)
        copy.start()
        copy.wait()


def band(steps, genotypes, pop_id, window, tile_counts, weights):
    snps = genotypes.shape[2]
    tiles = snps // TILE
    half = tiles // 2
    assert snps == WIN and tiles % 2 == 0 and lax.axis_size("pop") == 2
    plan = Plan(steps, tiles)
    behind = [(i + 1, i) for i in range(lax.axis_size("snp") - 1)]

    def swap(block, route):
        return lax.ppermute(block, "pop", route)

    both = [(0, 1), (1, 0)]
    arrivals = []
    for j, hop in enumerate(plan.hops):
        span = slice(hop.tile * TILE, (hop.tile + hop.wide) * TILE)
        if j == 0:
            piece = piece_part(genotypes, tile_counts, hop.wide)
        else:
            piece = genotypes[:, :, span] * valid[span]
        arrivals.append(lax.ppermute(piece, "snp", behind))
        if j == 0:
            ah, al, own0, own1, send, *more = own_part(plan, genotypes, tile_counts, pop_id, weights)
            swapped = [swap(send, both)] + [swap(x, both[1:]) for x in more]
            counts, send, piece = lax.optimization_barrier((tile_counts, send, piece))
            valid = (counts[:, None] > jnp.arange(TILE, dtype=jnp.int32)[None, :]).astype(F32).reshape(snps)
        else:
            valid, piece = lax.optimization_barrier((valid, piece))
    parts = []
    for j, (hop, got) in enumerate(zip(plan.hops, arrivals)):
        top, bottom, send = hop_part(plan, hop, got, ah, al, own0, j)
        route = both if hop.top or hop.rest[1] else both[:1]
        parts.append((top, bottom, swap(send, route)))
    lists = [own0, own1, *swapped]
    for part in parts[:-2]:
        lists += [x for x in part if x is not None]
    shape = jax.ShapeDtypeStruct((half * TILE, WIN), F32)
    anywhere = pl.BlockSpec(memory_space=pl.ANY)
    open_rows = tiles - plan.hops[-2].first
    finish = pl.pallas_call(
        functools.partial(finish_kernel, plan),
        in_specs=[SMEM] + [VMEM] * len(lists),
        out_specs=[anywhere, VMEM],
        out_shape=[shape, jax.ShapeDtypeStruct((open_rows, TILE, TILE), F32)],
        scratch_shapes=[
            pltpu.VMEM((half, steps + 1, TILE, TILE), F32),
            pltpu.VMEM((half * TILE, WIN), F32),
            pltpu.SemaphoreType.DMA((2 * half,)),
        ],
        cost_estimate=pl.CostEstimate(flops=10**9, bytes_accessed=6 * half * TILE * WIN * 4, transcendentals=0),
        compiler_params=PARAMS,
    )
    out, edge = finish(window, *lists)
    tile = jax.ShapeDtypeStruct((1, TILE, TILE), F32)
    cost = pl.CostEstimate(flops=10**7, bytes_accessed=6 * TILE * TILE * 4, transcendentals=0)
    out, ready = pl.pallas_call(
        functools.partial(next_kernel, plan),
        in_specs=[SMEM, anywhere] + [VMEM] * 3,
        out_specs=[anywhere, VMEM],
        out_shape=[shape, tile],
        input_output_aliases={1: 0},
        scratch_shapes=[
            pltpu.VMEM((open_rows, TILE, plan.hops[-2].wide * TILE), F32),
            pltpu.SemaphoreType.DMA((open_rows,)),
        ],
        cost_estimate=cost,
        compiler_params=PARAMS,
    )(window, out, edge, parts[-2][1], parts[-2][2])
    return pl.pallas_call(
        functools.partial(last_kernel, plan),
        in_specs=[SMEM, anywhere] + [VMEM] * 3,
        out_specs=anywhere,
        out_shape=shape,
        input_output_aliases={1: 0},
        scratch_shapes=[pltpu.VMEM((TILE, TILE), F32), pltpu.SemaphoreType.DMA],
        cost_estimate=cost,
        compiler_params=PARAMS,
    )(window, out, ready, parts[-1][1], parts[-1][2])


def solution(mesh):
    sizes = sorted(HOPS)

    def branch(steps):
        def body(*args):
            return band(steps, *args)

        return body

    def body(genotypes, pop_id, window, tile_counts, weights):
        steps = (window[0] + TILE - 1) // TILE
        return lax.switch(
            jnp.clip(steps - sizes[0], 0, len(sizes) - 1),
            [branch(n) for n in sizes],
            genotypes,
            pop_id,
            window,
            tile_counts,
            weights,
        )

    return jax.shard_map(
        body,
        mesh=mesh,
        in_specs=(P("pop", None, "snp"), P(), P(), P("snp"), P()),
        out_specs=P(("snp", "pop"), None),
        check_vma=False,
    )
```

```python
import functools

import jax
import jax.numpy as jnp
from jax import lax
from jax.experimental import pallas as pl
from jax.experimental.pallas import tpu as pltpu
from jax.sharding import PartitionSpec as P


WIN = 1024
TILE = 128
STRIP = 256
OWN_STRIP = 512
F32 = jnp.float32
BF16 = jnp.bfloat16
SMEM = pl.BlockSpec(memory_space=pltpu.SMEM)
VMEM = pl.BlockSpec(memory_space=pltpu.VMEM)
PARAMS = pltpu.CompilerParams(vmem_limit_bytes=20 * 2**20)
HOPS = {8: (2, 2, 2, 1, 1), 7: (2, 2, 1, 1, 1), 6: (2, 2, 1, 1), 5: (2, 2, 1)}


class Hop:
    def __init__(self, tile, wide, steps, tiles):
        self.tile, self.wide = tile, wide
        self.first = tile + tiles - steps
        self.base = max(self.first, tiles // 2)
        self.top = max(0, tiles // 2 - self.first) * wide
        self.bottom = (tiles - self.base) * wide
        self.rest = (0, 0)
        self.skip = 0

    def spot(self, row, base, w):
        if self.skip:
            return (row - base) * self.wide + self.wide - 1 - w - self.skip
        return (row - base) * self.wide + w


class Plan:
    def __init__(self, steps, tiles):
        self.steps, self.tiles, self.half = steps, tiles, tiles // 2
        self.counts = [min(steps + 1, tiles - r) for r in range(tiles)]
        starts = [sum(self.counts[:r]) for r in range(tiles + 1)]
        self.n0 = starts[self.half]
        self.n1 = starts[tiles] - self.n0
        self.starts = [s if r < self.half else s - self.n0 for r, s in enumerate(starts[:tiles])]
        self.hops, tile = [], 0
        for wide in HOPS[steps]:
            self.hops.append(Hop(tile, wide, steps, tiles))
            tile += wide
        assert self.hops[-2].first >= self.half
        assert self.hops[-1].first == tiles - 1 and self.hops[-1].wide == 1
        self.hops[-2].skip = self.hops[-2].wide - 1
        self.hops[-2].bottom -= self.hops[-2].skip
        spare = sum(max(0, hop.bottom - hop.top) for hop in self.hops[:-2])
        self.first_swap = max(self.n1, self.n0 - spare)
        self.even = self.n1 if steps == min(HOPS) else self.first_swap
        self.extra = self.first_swap - self.even
        self.late = self.hops[-2].wide > 1
        left = self.first_swap
        for hop in self.hops[:-2]:
            take = max(0, min(self.n0 - left, hop.bottom - hop.top))
            hop.rest = (left, take)
            hop.swap = max(hop.bottom, hop.top + take)
            left += take
        assert left == self.n0 or left == self.first_swap > self.n0


def split(x):
    high = x.astype(BF16)
    return high, (x - high.astype(F32)).astype(BF16)


def pick(row, values):
    result = values[0]
    for r, value in enumerate(values[1:], 1):
        result = jnp.where(row == r, value, result)
    return result


def piece_kernel(counts_ref, g_ref, out, counts, sems):
    cohorts, people, span = out.shape
    parts = (sems.shape[0] - 1) // cohorts
    rows = people // parts
    copies = []
    for i in range(cohorts * parts):
        c, k = i // parts, i % parts
        area = (c, pl.ds(k * rows, rows))
        copies.append(
            pltpu.make_async_copy(g_ref.at[area + (pl.ds(0, span),)], out.at[area], sems.at[i])
        )
        copies[-1].start()
    table = pltpu.make_async_copy(counts_ref, counts, sems.at[cohorts * parts])
    table.start()
    table.wait()
    lane = lax.broadcasted_iota(jnp.int32, (1, TILE), 1)
    mask = jnp.concatenate([(lane < counts[w]).astype(F32) for w in range(span // TILE)], axis=1)
    for i, copy in enumerate(copies):
        copy.wait()
        c, k = i // parts, i % parts

        def cut(j, carry, c=c, k=k):
            area = pl.ds(pl.multiple_of(k * rows + j * 128, 128), 128)
            out[c, area, :] = out[c, area, :] * mask
            return carry

        lax.fori_loop(0, rows // 128, cut, 0)


def piece_part(genotypes, tile_counts, wide):
    cohorts, people, _ = genotypes.shape
    return pl.pallas_call(
        piece_kernel,
        in_specs=[pl.BlockSpec(memory_space=pl.ANY)] * 2,
        out_specs=VMEM,
        out_shape=jax.ShapeDtypeStruct((cohorts, people, wide * TILE), F32),
        scratch_shapes=[pltpu.SMEM(tile_counts.shape, jnp.int32), pltpu.SemaphoreType.DMA((cohorts * 4 + 1,))],
        cost_estimate=pl.CostEstimate(flops=10**6, bytes_accessed=8 * cohorts * people * wide * TILE, transcendentals=0),
        compiler_params=PARAMS,
        name="piece",
    )(tile_counts, genotypes)


def own_kernel(plan, counts, pops, table, g_ref, ah, al, own0, own1, send, *refs):
    more = refs[0] if plan.extra else None
    high, low = refs[-2:]
    cohorts, people, span = g_ref.shape
    wide = span // TILE
    step = pl.program_id(0)
    group = lax.axis_index("pop")
    lane = lax.broadcasted_iota(jnp.int32, (1, TILE), 1)
    for w in range(wide):
        t = step * wide + w
        place = lax.axis_index("snp") * plan.tiles + t
        mask = (lane < counts[t]).astype(F32)
        total = table[pops[0], place]
        for e in range(1, pops.shape[0]):
            total = total + table[pops[e], place]
        rows = pl.ds(pl.multiple_of(t * TILE, TILE), TILE)
        columns = slice(w * TILE, (w + 1) * TILE)

        def prepare(i, carry):
            c, k = i // (people // OWN_STRIP), i % (people // OWN_STRIP)
            deep = pl.ds(pl.multiple_of(i * OWN_STRIP, OWN_STRIP), OWN_STRIP)
            x = g_ref[c, pl.ds(pl.multiple_of(k * OWN_STRIP, OWN_STRIP), OWN_STRIP), columns] * mask
            high[deep, columns], low[deep, columns] = split(x)
            share = table[pops[group * cohorts + c], place]
            coef = jnp.full((1, TILE), share, F32) / jnp.full((1, TILE), total, F32) * (1.0 / people)
            ah[rows, deep], al[rows, deep] = split((x * coef).T)
            return carry

        lax.fori_loop(0, cohorts * people // OWN_STRIP, prepare, 0)

    def block(q, carry):
        rows = pl.ds(pl.multiple_of(q * span, span), span)
        prod = jnp.dot(ah[rows, :], high[...], preferred_element_type=F32)
        prod = prod + jnp.dot(ah[rows, :], low[...], preferred_element_type=F32)
        prod = prod + jnp.dot(al[rows, :], high[...], preferred_element_type=F32)
        for k in range(wide):
            row = q * wide + k
            start = pick(row, plan.starts)
            for w in range(wide):
                m = step * wide + w - row
                spot = start + m
                inside = (m >= 0) & (m <= plan.steps)
                tile = prod[k * TILE : (k + 1) * TILE, w * TILE : (w + 1) * TILE]

                @pl.when(inside & (row < plan.half))
                def _():
                    own0[spot] = tile

                @pl.when(inside & (row >= plan.half))
                def _():
                    own1[spot] = tile

                other = inside & ((row < plan.half) == (group == 1))

                @pl.when(other & (spot < plan.even))
                def _():
                    send[spot] = tile

                if more is not None:

                    @pl.when(other & (spot >= plan.even) & (spot < plan.first_swap))
                    def _():
                        more[spot - plan.even] = tile

        return carry

    lax.fori_loop(jnp.maximum(step * wide - plan.steps, 0) // wide, step + 1, block, 0)


def own_part(plan, genotypes, tile_counts, pop_id, weights):
    cohorts, people, snps = genotypes.shape
    deep = cohorts * people
    span = 2 * TILE
    tall = jax.ShapeDtypeStruct((snps, deep), BF16)
    sizes = [plan.n0, plan.n1, plan.even] + ([plan.extra] if plan.extra else [])
    return pl.pallas_call(
        functools.partial(own_kernel, plan),
        grid=(snps // span,),
        in_specs=[SMEM, SMEM, SMEM, pl.BlockSpec((cohorts, people, span), lambda t: (0, 0, t))],
        out_specs=[VMEM] * (2 + len(sizes)),
        out_shape=[tall, tall] + [jax.ShapeDtypeStruct((n, TILE, TILE), F32) for n in sizes],
        scratch_shapes=[pltpu.VMEM((deep, span), BF16), pltpu.VMEM((deep, span), BF16)],
        cost_estimate=pl.CostEstimate(
            flops=6 * deep * snps * snps * 5 // 8, bytes_accessed=4 * deep * snps, transcendentals=0
        ),
        compiler_params=PARAMS,
    )(tile_counts, pop_id, weights, genotypes)


def hop_kernel(plan, hop, got, ah, al, *refs):
    refs = list(refs)
    own0 = refs.pop(0) if hop.rest[1] else None
    top = refs.pop(0) if hop.top else None
    bottom = refs.pop(0)
    low, high = refs.pop(), refs.pop()
    send = refs.pop() if refs else None
    group = lax.axis_index("pop")
    wide = hop.wide
    people = got.shape[1]

    def prepare(i, carry):
        c, k = i // (people // STRIP), i % (people // STRIP)
        deep = pl.ds(pl.multiple_of(i * STRIP, STRIP), STRIP)
        high[deep, :], low[deep, :] = split(got[c, pl.ds(pl.multiple_of(k * STRIP, STRIP), STRIP), :])
        return carry

    lax.fori_loop(0, got.shape[0] * people // STRIP, prepare, 0)

    def block(row, tall):
        rows = pl.ds(pl.multiple_of(row * TILE, TILE), tall * TILE)
        if wide == 1:
            both = jnp.concatenate([high[...], low[...]], axis=1)
            prod = jnp.dot(ah[rows, :], both, preferred_element_type=F32)
            prod = prod[:, :TILE] + prod[:, TILE:]
        else:
            prod = jnp.dot(ah[rows, :], high[...], preferred_element_type=F32)
            prod = prod + jnp.dot(ah[rows, :], low[...], preferred_element_type=F32)
        prod = prod + jnp.dot(al[rows, :], high[...], preferred_element_type=F32)
        for k in range(tall):

            def put(out, base, owner):
                for w in range(wide):
                    tile = prod[k * TILE : (k + 1) * TILE, w * TILE : (w + 1) * TILE]
                    spot = hop.spot(row + k, base, w)
                    if hop.skip:

                        @pl.when(spot >= 0)
                        def _():
                            out[spot] = tile

                    else:
                        out[spot] = tile
                    if send is not None:

                        @pl.when(group == owner)
                        def _():
                            send[spot] = tile

            if top is not None:
                upper = (row + k >= hop.first) & (row + k < plan.half)
                pl.when(upper)(functools.partial(put, top, hop.first, 1))
            pl.when(row + k >= hop.base)(functools.partial(put, bottom, hop.base, 0))

    tall = min(wide, 2)

    def pair(q, carry):
        block(tall * q, tall)
        return carry

    if plan.tiles - hop.first > 1:
        lax.fori_loop(hop.first // tall, plan.tiles // tall, pair, 0)
    else:
        block(hop.first, 1)
    if hop.rest[1]:

        @pl.when(group == 1)
        def _():
            send[hop.top : hop.top + hop.rest[1]] = own0[hop.rest[0] : hop.rest[0] + hop.rest[1]]


def hop_part(plan, hop, got, ah, al, own0, tag):
    deep = ah.shape[1]
    span = hop.wide * TILE
    args = [got, ah, al] + ([own0] if hop.rest[1] else [])
    sizes = ([hop.top] if hop.top else []) + [hop.bottom] + ([hop.swap] if tag + 2 < len(plan.hops) else [])
    outs = pl.pallas_call(
        functools.partial(hop_kernel, plan, hop),
        in_specs=[VMEM] * len(args),
        out_specs=[VMEM] * len(sizes),
        out_shape=[jax.ShapeDtypeStruct((n, TILE, TILE), F32) for n in sizes],
        scratch_shapes=[pltpu.VMEM((deep, span), BF16), pltpu.VMEM((deep, span), BF16)],
        cost_estimate=pl.CostEstimate(
            flops=6 * deep * span * (plan.tiles - hop.first) * TILE,
            bytes_accessed=4 * deep * span,
            transcendentals=0,
        ),
        compiler_params=PARAMS,
    )(*args)
    outs = list(outs)
    top = outs.pop(0) if hop.top else None
    return top, outs[0], outs[-1]


def skew(tiles, group):
    rows = tiles[0].shape[0]
    low = lax.broadcasted_iota(jnp.int32, (8, TILE), 0)
    row = lax.broadcasted_iota(jnp.int32, (rows, TILE), 0)
    result = []
    for tile in tiles:
        parts = []
        for g in range(rows // 8):
            part = tile[8 * g : 8 * g + 8]
            shift = 2 * TILE - 8 * g - group * 8
            near, far = pltpu.roll(part, shift % TILE, 1), pltpu.roll(part, (shift - 4) % TILE, 1)
            parts.append(jnp.where(low >= 4, far, near))
        result.append(jnp.concatenate(parts, axis=0))
    for bit in (1, 2):
        odd = (row & bit) != 0
        result = [jnp.where(odd, pltpu.roll(tile, TILE - bit, 1), tile) for tile in result]
    return result


def band_tiles(tiles, first, group, window):
    shape = tiles[0].shape
    lane = lax.broadcasted_iota(jnp.int32, shape, 1)
    near = lane + lax.broadcasted_iota(jnp.int32, shape, 0) + group * 8 < TILE
    for m, (this, after) in enumerate(zip(tiles, tiles[1:]), first):
        yield jnp.where(m * TILE + lane < window, jnp.where(near, this, after), 0.0)


def runs(plan, h, r, own, swapped, parts):
    row = h * plan.half + r
    start, count = plan.starts[row], plan.counts[row]
    result = []
    edges = [(swapped[0], 0, plan.even, 0)]
    if h == 0:
        edges += [(more, plan.even, plan.extra, 0) for more in swapped[1:]]
        edges += [(part[2], hop.rest[0], hop.rest[1], hop.top) for hop, part in zip(plan.hops, parts)]
    for came, begin, length, base in edges:
        lo, hi = max(start, begin), min(start + count, begin + length)
        if lo < hi:
            result.append((own[h], lo, came, base + lo - begin, lo - start, hi - lo))
    for hop, (top, bottom, came) in zip(plan.hops, parts):
        if row < hop.first:
            continue
        step = plan.tiles + hop.tile - row
        spot = (row - (hop.base if h else hop.first)) * hop.wide
        result.append((bottom if h else top, spot, came, spot, step, min(hop.wide, plan.steps + 1 - step)))
    return result


def finish_kernel(plan, window, own0, own1, *refs):
    refs = list(refs)
    swapped = [refs.pop(0) for _ in range(2 if plan.extra else 1)]
    sems, lines, band, edge, out = (refs.pop() for _ in range(5))
    parts = []
    for hop in plan.hops[:-2]:
        top = refs.pop(0) if hop.top else None
        parts.append((top, refs.pop(0), refs.pop(0)))
    group = lax.axis_index("pop")
    for h in range(2):

        @pl.when(group == h)
        def _():
            for r in range(plan.half):
                for kept, a, came, b, step, count in runs(plan, h, r, (own0, own1), swapped, parts):

                    def add(i, carry, r=r, kept=kept, a=a, came=came, b=b, step=step):
                        band[r, step + i] = kept[a + i] + came[b + i]
                        return carry

                    lax.fori_loop(0, count, add, 0)

    for i in range(edge.shape[0]):
        row = plan.hops[-2].first + i
        edge[i] = band[row - plan.half, plan.tiles + plan.hops[-2].tile - row - 1]

    strip = TILE
    strips = TILE // strip

    def line(i, carry):
        r, q = i // strips, i % strips
        inner = pl.ds(pl.multiple_of(q * strip, strip), strip)
        rows = pl.ds(pl.multiple_of(i * strip, strip), strip)
        tiles = skew([band[r, m, inner, :] for m in range(plan.steps + 1)], q * (strip // 8))
        for m, tile in enumerate(band_tiles(tiles, 0, q * (strip // 8), window[0])):
            lines[rows, m * TILE : (m + 1) * TILE] = tile
        if plan.steps * TILE < out.shape[1]:
            lines[rows, plan.steps * TILE :] = jnp.zeros((strip, out.shape[1] - plan.steps * TILE), F32)
        leave(i).start()
        return carry

    def leave(i):
        rows = pl.ds(pl.multiple_of(i * strip, strip), strip)
        return pltpu.make_async_copy(lines.at[rows, :], out.at[rows, :], sems.at[i])

    lax.fori_loop(0, plan.half * strips, line, 0)
    for i in range(plan.half * strips):
        leave(i).wait()


def next_kernel(plan, window, old, edge, kept, came, out, ready, fresh, sems):
    del old
    hop = plan.hops[-2]

    @pl.when(lax.axis_index("pop") == 1)
    def _():
        copies = []
        for i in range(edge.shape[0]):
            row = hop.first + i
            step = plan.tiles + hop.tile - row
            tiles = [edge[i]]
            for w in range(min(hop.wide, plan.steps + 1 - step)):
                spot = hop.spot(i, 0, w)
                tiles.append(kept[spot] + came[spot])
            tiles = skew(tiles, 0)
            for m, tile in enumerate(band_tiles(tiles, step - 1, 0, window[0])):
                fresh[i, :, m * TILE : (m + 1) * TILE] = tile
            width = (len(tiles) - 1) * TILE
            copies.append(
                pltpu.make_async_copy(
                    fresh.at[i, :, pl.ds(0, width)],
                    out.at[pl.ds((row - plan.half) * TILE, TILE), pl.ds((step - 1) * TILE, width)],
                    sems.at[i],
                )
            )
            copies[-1].start()
        ready[0] = tiles[-1]
        for copy in copies:
            copy.wait()


def last_kernel(plan, window, old, ready, kept, came, out, fresh, sem):
    del old

    @pl.when(lax.axis_index("pop") == 1)
    def _():
        total = kept[0] + came[0] if plan.late else came[0, 0] + came[1, 0]
        tiles = [ready[0]] + skew([total], 0)
        (fresh[...],) = band_tiles(tiles, plan.steps - 1, 0, window[0])
        corner = out.at[pl.ds((plan.half - 1) * TILE, TILE), pl.ds((plan.steps - 1) * TILE, TILE)]
        copy = pltpu.make_async_copy(fresh, corner, sem)
        copy.start()
        copy.wait()


def band(steps, genotypes, pop_id, window, tile_counts, weights):
    snps = genotypes.shape[2]
    tiles = snps // TILE
    half = tiles // 2
    assert snps == WIN and tiles % 2 == 0 and lax.axis_size("pop") == 2
    plan = Plan(steps, tiles)
    behind = [(i + 1, i) for i in range(lax.axis_size("snp") - 1)]

    def swap(block, route):
        return lax.ppermute(block, "pop", route)

    both = [(0, 1), (1, 0)]
    arrivals = []
    for j, hop in enumerate(plan.hops):
        span = slice(hop.tile * TILE, (hop.tile + hop.wide) * TILE)
        if j == 0:
            piece = piece_part(genotypes, tile_counts, hop.wide)
        else:
            piece = genotypes[:, :, span] * valid[span]
        arrivals.append(lax.ppermute(piece, "snp", behind))
        if j == 0:
            ah, al, own0, own1, send, *more = own_part(plan, genotypes, tile_counts, pop_id, weights)
            swapped = [swap(send, both)] + [swap(x, both[1:]) for x in more]
            counts, send, piece = lax.optimization_barrier((tile_counts, send, piece))
            valid = (counts[:, None] > jnp.arange(TILE, dtype=jnp.int32)[None, :]).astype(F32).reshape(snps)
        else:
            valid, piece = lax.optimization_barrier((valid, piece))
    parts = []
    for j, (hop, got) in enumerate(zip(plan.hops, arrivals)):
        top, bottom, send = hop_part(plan, hop, got, ah, al, own0, j)
        route = both if hop.top or hop.rest[1] else both[:1]
        if j + 1 < len(plan.hops) or plan.late:
            parts.append((top, bottom, swap(send, route)))
        else:
            parts.append((top, bottom, lax.all_gather(bottom, "pop")))
    lists = [own0, own1, *swapped]
    for part in parts[:-2]:
        lists += [x for x in part if x is not None]
    shape = jax.ShapeDtypeStruct((half * TILE, WIN), F32)
    anywhere = pl.BlockSpec(memory_space=pl.ANY)
    open_rows = tiles - plan.hops[-2].first
    finish = pl.pallas_call(
        functools.partial(finish_kernel, plan),
        in_specs=[SMEM] + [VMEM] * len(lists),
        out_specs=[anywhere, VMEM],
        out_shape=[shape, jax.ShapeDtypeStruct((open_rows, TILE, TILE), F32)],
        scratch_shapes=[
            pltpu.VMEM((half, steps + 1, TILE, TILE), F32),
            pltpu.VMEM((half * TILE, WIN), F32),
            pltpu.SemaphoreType.DMA((half,)),
        ],
        cost_estimate=pl.CostEstimate(flops=10**9, bytes_accessed=6 * half * TILE * WIN * 4, transcendentals=0),
        compiler_params=PARAMS,
    )
    out, edge = finish(window, *lists)
    tile = jax.ShapeDtypeStruct((1, TILE, TILE), F32)
    cost = pl.CostEstimate(flops=10**7, bytes_accessed=6 * TILE * TILE * 4, transcendentals=0)
    out, ready = pl.pallas_call(
        functools.partial(next_kernel, plan),
        in_specs=[SMEM, anywhere] + [VMEM] * 3,
        out_specs=[anywhere, VMEM],
        out_shape=[shape, tile],
        input_output_aliases={1: 0},
        scratch_shapes=[
            pltpu.VMEM((open_rows, TILE, plan.hops[-2].wide * TILE), F32),
            pltpu.SemaphoreType.DMA((open_rows,)),
        ],
        cost_estimate=cost,
        compiler_params=PARAMS,
    )(window, out, edge, parts[-2][1], parts[-2][2])
    return pl.pallas_call(
        functools.partial(last_kernel, plan),
        in_specs=[SMEM, anywhere] + [VMEM] * 3,
        out_specs=anywhere,
        out_shape=shape,
        input_output_aliases={1: 0},
        scratch_shapes=[pltpu.VMEM((TILE, TILE), F32), pltpu.SemaphoreType.DMA],
        cost_estimate=cost,
        compiler_params=PARAMS,
    )(window, out, ready, parts[-1][1], parts[-1][2])


def solution(mesh):
    sizes = sorted(HOPS)

    def branch(steps):
        def body(*args):
            return band(steps, *args)

        return body

    def body(genotypes, pop_id, window, tile_counts, weights):
        steps = (window[0] + TILE - 1) // TILE
        return lax.switch(
            jnp.clip(steps - sizes[0], 0, len(sizes) - 1),
            [branch(n) for n in sizes],
            genotypes,
            pop_id,
            window,
            tile_counts,
            weights,
        )

    return jax.shard_map(
        body,
        mesh=mesh,
        in_specs=(P("pop", None, "snp"), P(), P(), P("snp"), P()),
        out_specs=P(("snp", "pop"), None),
        check_vma=False,
    )
```
